512 devices in a mesh: scen: 64 (over z, y), fac: 8 (over x, core).
Axes of the slice: x: 4, y: 8, z: 8, core: 2. Of those that a mesh axis runs over, the one named last changes fastest.
Arguments:
- scenario_pnl: float32 [65536, 2048], P('scen', 'fac'), may hold values from -300 to 300
Outputs:
- covariance: float32 [2048, 2048], P('scen', 'fac')
- factor_means: float32 [2048], P('fac')
The draws below stay inside these ranges and needn't reach their ends.
All inputs are finite; a program needn't handle non-finite values.
Results may differ from the reference program's by a relative error of at most 0.0003.
Values sent between devices are 32-bit elements; how exact they have to be, the bound alone decides.
No kernel may reach another device: no remote copies, remote signals or barrier semaphores. Data moves between devices by JAX's collectives and lax.ppermute only.
A program may use at most 64 MiB of HBM per device.

```python
import jax
import jax.numpy as jnp
from jax import lax

F = 2048
SCENARIOS = 65536


def draw_scenario_pnl(key, part):
    keys = jax.random.split(jax.random.fold_in(key, 11), 9)
    noise = jnp.clip(jax.random.normal(keys[0], (SCENARIOS, F), jnp.float32), -4.0, 4.0)
    first = jax.random.permutation(keys[1], F)
    second = jax.random.permutation(keys[2], F)
    mixed = noise + 0.5 * noise[:, first] + 0.5 * noise[:, second]
    levels = jnp.clip(0.8 * jax.random.normal(keys[3], (F,), jnp.float32), -2.0, 2.0)
    scales = jnp.exp(jax.random.uniform(keys[4], (F,), jnp.float32, jnp.log(0.4), jnp.log(2.5)))
    drift = 0.5 + jnp.arange(SCENARIOS, dtype=jnp.float32) / SCENARIOS
    drawn = scales[None, :] * (mixed + drift[:, None] * levels[None, :])
    chosen = jax.random.permutation(keys[6], F) < F // 8
    signs = jnp.where(jax.random.uniform(keys[7], (F,), jnp.float32) < 0.5, -1.0, 1.0)
    offsets = signs * jax.random.uniform(keys[8], (F,), jnp.float32, 200.0, 260.0)
    shifted = offsets[None, :] + mixed + 2.0 * (drift[:, None] - 1.0)
    return jnp.where(chosen[None, :], shifted, drawn)


def setup_inputs(seed: int = 0) -> dict:
    key_of = jax.random.split(jax.random.key(seed), 2)
    return {
        "scenario_pnl": draw_scenario_pnl(jax.random.fold_in(key_of[1], 71), 0),
    }


def reference(scenario_pnl):
    count = scenario_pnl.shape[0]
    factor_means = jnp.sum(scenario_pnl, axis=0) / count
    centered = scenario_pnl - factor_means[None, :]
    product = lax.dot_general(centered, centered, (((0,), (0,)), ((), ())), precision=lax.Precision.HIGHEST, preferred_element_type=jnp.float32)
    covariance = product / (count - 1)
    return covariance, factor_means
```

```python
import functools

import jax
import jax.numpy as jnp
from jax import lax
from jax.experimental import pallas as pl
from jax.experimental.pallas import tpu as pltpu
from jax.sharding import Mesh
from jax.sharding import PartitionSpec as P

SCEN = ("z1", "z0", "y1", "y0")
FAC = ("x", "c")
VMEM = pl.BlockSpec(memory_space=pltpu.VMEM)
F32 = jnp.float32
BF16 = jnp.bfloat16


def shape(*dims, dtype=F32):
    return jax.ShapeDtypeStruct(dims, dtype)


def outer(left, right):
    return lax.dot_general(
        left,
        right,
        (((0,), (0,)), ((), ())),
        precision=lax.Precision.HIGHEST,
        preferred_element_type=F32,
    )


def centre_kernel(x_ref, a_ref, b_ref):
    rows, cols = x_ref.shape
    half = rows // 2
    mean = jnp.sum(x_ref[...], axis=0, keepdims=True) * (1.0 / rows)
    a_ref[0:half, :] = x_ref[0:half, :] - mean
    a_ref[half : half + 8, :] = jnp.broadcast_to(mean, (8, cols))
    b_ref[...] = x_ref[half:rows, :] - mean


def turn_kernel(a_ref, b_ref, t_ref):
    half, cols = b_ref.shape
    for ref, at in ((a_ref, 0), (b_ref, half)):
        turned = ref[0:half, :].T
        high = turned.astype(BF16)
        t_ref[0:cols, at : at + half] = high
        t_ref[cols : 2 * cols, at : at + half] = (turned - high.astype(F32)).astype(BF16)


def gram_kernel(n, own_a, t_ref, *refs):
    pieces, outs, (block, mean) = refs[: 4 * n], refs[4 * n : 4 * n + 4], refs[4 * n + 4 :]
    half = refs[1].shape[0]
    cols = t_ref.shape[0] // 2
    z0, y0, c = lax.axis_index("z0"), lax.axis_index("y0"), lax.axis_index("c")
    for k in range(n):
        for swapped in range(2):
            core = (1 - c) if swapped else c
            total = None
            for part in range(2):
                ref = pieces[4 * k + 2 * swapped + part]
                left = ref[0:half, :]
                high = left.astype(BF16)
                low = (left - high.astype(F32)).astype(BF16)
                at = part * half
                both = jnp.dot(t_ref[:, at : at + half], high, preferred_element_type=F32)
                rest = jnp.dot(t_ref[0:cols, at : at + half], low, preferred_element_type=F32)
                here = both[0:cols] + (both[cols:] + rest)
                total = here if total is None else total + here
            block[core] = total.T.reshape(4, 2, 32, cols)
            mean[core] = pieces[4 * k + 2 * swapped][half : half + 8, :]
        for r in range(4):
            dz, dy = divmod(r, 2)
            zt = (1 - z0) if dz else z0
            yt = (1 - y0) if dy else y0
            for y1 in range(4):
                at = (4 * k + y1) * 32
                outs[r][at : at + 32, :] = block[zt, y1, yt]
            outs[r][128 * n + 1 + k : 128 * n + 2 + k, :] = mean[zt, 0:1, :]
    for r in range(4):
        outs[r][128 * n : 128 * n + 1, :] = own_a[half : half + 1, :]
        outs[r][128 * n + 1 + n : 128 * n + 8, :] = jnp.zeros((7 - n, cols), F32)


def merge_block_kernel(count, *refs):
    first, second, out_ref, shift = refs[0:4], refs[4:8], refs[8], refs[9]
    cols = out_ref.shape[-1]
    x, y0 = lax.axis_index("x"), lax.axis_index("y0")
    own = [r[384:385, :] for r in first]
    own_mean = (own[0] + own[1] + own[2] + own[3]) * 0.25
    zeros = jnp.zeros((4, cols), F32)
    right = jnp.concatenate([m - own_mean for m in own] + [zeros], axis=0)
    for k, step in enumerate((0, 1, 3, 2)):
        group, at, row = (first, 128 * k, 385 + k) if k < 3 else (second, 0, 129)
        means = [r[row : row + 1, :] for r in group]
        mean = (means[0] + means[1] + means[2] + means[3]) * 0.25
        left = jnp.concatenate([m - mean for m in means] + [zeros], axis=0)
        shift[...] = (outer(left, right) * float(count)).reshape(4, 2, 32, cols)
        to = lax.rem(x + step, 4)
        for y1 in range(4):
            lo = at + 32 * y1
            total = (group[0][lo : lo + 32, :] + group[1][lo : lo + 32, :]) + (
                group[2][lo : lo + 32, :] + group[3][lo : lo + 32, :]
            )
            out_ref[4 * to + y1, 0:32, :] = total + shift[y1, y0]
            out_ref[4 * to + y1, 32:33, :] = own_mean
            out_ref[4 * to + y1, 33:34, :] = mean
            out_ref[4 * to + y1, 34:40, :] = jnp.zeros((6, cols), F32)


def merge_all_kernel(count, in_ref, cov_ref, mean_ref, shift):
    blocks, _, cols = in_ref.shape
    total = in_ref[0, 0:32, :]
    for s in range(1, blocks):
        total = total + in_ref[s, 0:32, :]
    own = jnp.concatenate([in_ref[s, 32:33, :] for s in range(blocks)], axis=0)
    other = jnp.concatenate([in_ref[s, 33:34, :] for s in range(blocks)], axis=0)
    own_mean = jnp.sum(own, axis=0, keepdims=True) * (1.0 / blocks)
    other_mean = jnp.sum(other, axis=0, keepdims=True) * (1.0 / blocks)
    y = 2 * lax.axis_index("y1") + lax.axis_index("y0")
    shift[...] = (outer(other - other_mean, own - own_mean) * float(count)).reshape(8, 32, cols)
    cov_ref[...] = (total + shift[y]) / float(count * blocks - 1)
    mean_ref[...] = own_mean


def call(kernel, outs, args, scratch=()):
    return pl.pallas_call(
        kernel,
        out_shape=outs,
        in_specs=[VMEM] * len(args),
        out_specs=jax.tree.map(lambda _: VMEM, outs),
        scratch_shapes=scratch,
    )(*args)


def shifted(piece, axis, by):
    size = lax.axis_size(axis)
    return lax.ppermute(piece, axis, [(i, (i + by) % size) for i in range(size)])


def neighbour(piece, r):
    return lax.ppermute(piece, ("z0", "y0"), [(i, i ^ r) for i in range(4)])


def on_device(x):
    rows, cols = x.shape
    half = rows // 2
    a, b = call(centre_kernel, (shape(half + 8, cols), shape(half, cols)), (x,))
    up_a = shifted(a, "x", -1)
    down_b = shifted(b, "x", 1)
    up_b = shifted(b, "x", -1)
    down_a = shifted(a, "x", 1)
    far_a = shifted(up_a, "x", -1)
    far_b = shifted(down_b, "x", 1)
    t = call(turn_kernel, shape(2 * cols, rows, dtype=BF16), (a, b))

    def with_swapped(pa, pb):
        return (pa, pb, shifted(pa, "c", 1), shifted(pb, "c", 1))

    def gram(chips):
        n = len(chips)
        pieces = [p for chip in chips for p in with_swapped(*chip)]
        return call(
            functools.partial(gram_kernel, n),
            (shape(128 * n + 8, cols),) * 4,
            (a, t, *pieces),
            (pltpu.VMEM((2, 4, 2, 32, cols), F32), pltpu.VMEM((2, 8, cols), F32)),
        )

    first = gram([(a, b), (up_a, up_b), (down_a, down_b)])
    second = gram([(far_a, far_b)])
    sums = [first[0]] + [neighbour(first[r], r) for r in (1, 2, 3)]
    sums += [second[0]] + [neighbour(second[r], r) for r in (1, 2, 3)]
    block = call(
        functools.partial(merge_block_kernel, rows),
        shape(16, 40, cols),
        sums,
        (pltpu.VMEM((4, 2, 32, cols), F32),),
    )
    block = lax.all_to_all(block, ("z1", "y1"), 0, 0, tiled=True)
    covariance, mean = call(
        functools.partial(merge_all_kernel, 4 * rows),
        (shape(32, cols), shape(1, cols)),
        (block,),
        (pltpu.VMEM((8, 32, cols), F32),),
    )
    return covariance, mean.reshape(cols)


def solution(mesh):
    finer = Mesh(mesh.devices.reshape(4, 2, 4, 2, 4, 2), SCEN + FAC)
    return jax.shard_map(
        on_device,
        mesh=finer,
        in_specs=(P(SCEN, FAC),),
        out_specs=(P(SCEN, FAC), P(FAC)),
        check_vma=False,
    )
```

```python
import functools

import jax
import jax.numpy as jnp
from jax import lax
from jax.experimental import pallas as pl
from jax.experimental.pallas import tpu as pltpu
from jax.sharding import Mesh
from jax.sharding import PartitionSpec as P

SCEN = ("z1", "z0", "y1", "y0")
FAC = ("x", "c")
VMEM = pl.BlockSpec(memory_space=pltpu.VMEM)
F32 = jnp.float32
BF16 = jnp.bfloat16


def shape(*dims, dtype=F32):
    return jax.ShapeDtypeStruct(dims, dtype)


def outer(left, right):
    return lax.dot_general(
        left,
        right,
        (((0,), (0,)), ((), ())),
        precision=lax.Precision.HIGHEST,
        preferred_element_type=F32,
    )


def centre_kernel(x_ref, d_ref):
    rows, cols = x_ref.shape
    mean = jnp.sum(x_ref[...], axis=0, keepdims=True) * (1.0 / rows)
    d_ref[0:rows, :] = x_ref[...] - mean
    d_ref[rows : rows + 8, :] = jnp.broadcast_to(mean, (8, cols))


def turn(piece, t_ref, at):
    cols = piece.shape[1]
    turned = piece.T
    high = turned.astype(BF16)
    t_ref[at : at + cols, :] = high
    t_ref[at + 2 * cols : at + 3 * cols, :] = (turned - high.astype(F32)).astype(BF16)


def split(left):
    high = left.astype(BF16)
    return high, (left - high.astype(F32)).astype(BF16)


def against(t_ref, left, at, rows):
    high, low = split(left)
    two = t_ref.shape[0] // 2
    both = jnp.dot(t_ref[:, at : at + rows], high, preferred_element_type=F32)
    rest = jnp.dot(t_ref[0:two, at : at + rows], low, preferred_element_type=F32)
    return both[0:two] + (both[two:] + rest)


def place(total, block, c):
    cols = total.shape[1]
    block[c] = total[0:cols].T.reshape(4, 2, 32, cols)
    block[1 - c] = total[cols:].T.reshape(4, 2, 32, cols)


def deal(block, outs, at):
    z0, y0 = lax.axis_index("z0"), lax.axis_index("y0")
    for r in range(4):
        dy, b = divmod(r, 2)
        core = (1 - z0) if b else z0
        to = (1 - y0) if dy else y0
        for y1 in range(4):
            outs[r][at + 32 * y1 : at + 32 * y1 + 32, :] = block[core, y1, to]


def own_kernel(d_ref, s_ref, t_ref, *refs):
    outs, block = refs[:4], refs[4]
    cols = d_ref.shape[1]
    rows = d_ref.shape[0] - 8
    c = lax.axis_index("c")
    turn(d_ref[0:rows, :], t_ref, 0)
    turn(s_ref[0:rows, :], t_ref, cols)
    place(against(t_ref, d_ref[0:rows, :], 0, rows), block, c)
    deal(block, outs, 0)


def near_kernel(t_ref, d_ref, s_ref, up_ref, down_ref, *refs):
    own, outs, (block, mean) = refs[:4], refs[4:8], refs[8:]
    cols = d_ref.shape[1]
    rows = d_ref.shape[0] - 8
    z0, c = lax.axis_index("z0"), lax.axis_index("c")
    for k, ref in ((1, up_ref), (2, down_ref)):
        place(against(t_ref, ref[0:rows, :], 0, rows), block, c)
        deal(block, outs, 128 * k)
    mean[c] = d_ref[rows : rows + 8, :]
    mean[1 - c] = s_ref[rows : rows + 8, :]
    for r in range(4):
        core = (1 - z0) if r % 2 else z0
        outs[r][0:128, :] = own[r][...]
        outs[r][384:385, :] = mean[core, 0:1, :]
        for k, ref in enumerate((d_ref, up_ref, down_ref)):
            outs[r][385 + k : 386 + k, :] = ref[rows : rows + 1, :]
        outs[r][388:392, :] = jnp.zeros((4, cols), F32)


def far_kernel(t_ref, a_ref, b_ref, *refs):
    outs, block = refs[:4], refs[4]
    half = a_ref.shape[0]
    cols = a_ref.shape[1]
    c = lax.axis_index("c")
    total = against(t_ref, a_ref[...], 0, half) + against(t_ref, b_ref[0:half, :], half, half)
    place(total, block, c)
    deal(block, outs, 0)
    for r in range(4):
        outs[r][128:136, :] = b_ref[half : half + 8, :]


def merge_block_kernel(count, *refs):
    first, second, out_ref, shift = refs[0:5], refs[5:10], refs[10], refs[11]
    cols = shift.shape[-1]
    x, z0, y0, c = (lax.axis_index(n) for n in ("x", "z0", "y0", "c"))
    kept = jnp.full((1, cols), z0 == c)

    def read(group, lo, n):
        home = jnp.where(kept, group[0][lo : lo + n, :], group[1][lo : lo + n, :])
        return [home] + [r[lo : lo + n, :] for r in group[2:]]

    own = read(first, 384, 1)
    own_mean = (own[0] + own[1] + own[2] + own[3]) * 0.25
    zeros = jnp.zeros((4, cols), F32)
    right = jnp.concatenate([m - own_mean for m in own] + [zeros], axis=0)
    for k, step in enumerate((0, 1, 3, 2)):
        group, at, row = (first, 128 * k, 385 + k) if k < 3 else (second, 0, 128)
        means = read(group, row, 1)
        mean = (means[0] + means[1] + means[2] + means[3]) * 0.25
        left = jnp.concatenate([m - mean for m in means] + [zeros], axis=0)
        shift[...] = (outer(left, right) * float(count)).reshape(4, 2, 32, cols)
        to = lax.rem(x + step, 4)
        for y1 in range(4):
            parts = read(group, at + 32 * y1, 32)
            total = (parts[0] + parts[1]) + (parts[2] + parts[3]) + shift[y1, y0]
            for g in range(4):
                out_ref[4 * to + y1, :, cols * g : cols * g + cols] = total[8 * g : 8 * g + 8, :]
            for row, m in ((0, own_mean), (2, mean)):
                for h in range(2):
                    out_ref[4 * to + y1, row + h : row + h + 1, 4 * cols :] = m[:, 128 * h : 128 * h + 128]
            out_ref[4 * to + y1, 4:8, 4 * cols :] = jnp.zeros((4, 128), F32)


def merge_all_kernel(count, in_ref, cov_ref, mean_ref, shift):
    blocks = in_ref.shape[0]
    cols = cov_ref.shape[1]
    total = in_ref[0]
    for s in range(1, blocks):
        total = total + in_ref[s]

    def means(row):
        halves = [
            jnp.concatenate([in_ref[s, row + h : row + h + 1, 4 * cols :] for s in range(blocks)], axis=0)
            for h in range(2)
        ]
        return jnp.concatenate(halves, axis=1)

    own, other = means(0), means(2)
    own_mean = jnp.sum(own, axis=0, keepdims=True) * (1.0 / blocks)
    other_mean = jnp.sum(other, axis=0, keepdims=True) * (1.0 / blocks)
    y = 2 * lax.axis_index("y1") + lax.axis_index("y0")
    shift[...] = (outer(other - other_mean, own - own_mean) * float(count)).reshape(8, 4, 8, cols)
    for g in range(4):
        here = total[:, cols * g : cols * g + cols] + shift[y, g]
        cov_ref[8 * g : 8 * g + 8, :] = here / float(count * blocks - 1)
    mean_ref[...] = own_mean


def call(kernel, outs, args, scratch=(), mib=16, flops=0, moved=0):
    return pl.pallas_call(
        kernel,
        out_shape=outs,
        in_specs=[VMEM] * len(args),
        out_specs=jax.tree.map(lambda _: VMEM, outs),
        scratch_shapes=scratch,
        compiler_params=pltpu.CompilerParams(vmem_limit_bytes=mib * 2**20),
        cost_estimate=pl.CostEstimate(flops=flops, bytes_accessed=moved, transcendentals=0),
    )(*args)


def shifted(piece, axis, by):
    size = lax.axis_size(axis)
    return lax.ppermute(piece, axis, [(i, (i + by) % size) for i in range(size)])


def dealt(piece, r):
    pairs = []
    for i in range(8):
        z0, y0, c = i // 4, i // 2 % 2, i % 2
        j = c * 4 + (y0 ^ (r // 2)) * 2 + (z0 ^ (r % 2))
        if i != j:
            pairs.append((i, j))
    return lax.ppermute(piece, ("z0", "y0", "c"), pairs)


def on_device(x):
    rows, cols = x.shape
    half = rows // 2
    d = call(centre_kernel, shape(rows + 8, cols), (x,), flops=10**9, moved=2**21)
    up = shifted(d, "x", -1)
    down = shifted(d, "x", 1)
    swap = shifted(d, "c", 1)
    far_a = shifted(up[:half], "x", -1)
    far_b = shifted(down[half:], "x", 1)
    block = pltpu.VMEM((2, 4, 2, 32, cols), F32)
    t, *own = call(
        own_kernel,
        (shape(4 * cols, rows, dtype=BF16), *[shape(128, cols)] * 4),
        (d, swap),
        (block,),
        flops=2 * 10**9,
        moved=2**22,
    )
    near = call(
        near_kernel,
        [shape(392, cols)] * 4,
        (t, d, swap, up, down, *own),
        (block, pltpu.VMEM((2, 8, cols), F32)),
        flops=4 * 10**9,
        moved=2**22,
    )
    far = call(far_kernel, [shape(136, cols)] * 4, (t, far_a, far_b), (block,), flops=2 * 10**9, moved=2**22)
    sums = [near[0]] + [dealt(near[r], r) for r in range(4)]
    sums += [far[0]] + [dealt(far[r], r) for r in range(4)]
    merged = call(
        functools.partial(merge_block_kernel, rows),
        shape(16, 8, 4 * cols + 128),
        sums,
        (pltpu.VMEM((4, 2, 32, cols), F32),),
        flops=10**9,
        moved=2**22,
    )
    merged = lax.all_to_all(merged, ("z1", "y1"), 0, 0, tiled=True)
    covariance, mean = call(
        functools.partial(merge_all_kernel, 4 * rows),
        (shape(32, cols), shape(1, cols)),
        (merged,),
        (pltpu.VMEM((8, 4, 8, cols), F32),),
        flops=10**9,
        moved=2**20,
    )
    return covariance, mean.reshape(cols)


def solution(mesh):
    finer = Mesh(mesh.devices.reshape(4, 2, 4, 2, 4, 2), SCEN + FAC)
    return jax.shard_map(
        on_device,
        mesh=finer,
        in_specs=(P(SCEN, FAC),),
        out_specs=(P(SCEN, FAC), P(FAC)),
        check_vma=False,
    )
```

```python
import functools

import jax
import jax.numpy as jnp
from jax import lax
from jax.experimental import pallas as pl
from jax.experimental.pallas import tpu as pltpu
from jax.sharding import Mesh
from jax.sharding import PartitionSpec as P


SCEN = ("z1", "z0", "y1", "y0")
FAC = ("x", "c")
VMEM = pl.BlockSpec(memory_space=pltpu.VMEM)
F32 = jnp.float32
BF16 = jnp.bfloat16


def shape(*dims, dtype=F32):
    return jax.ShapeDtypeStruct(dims, dtype)


def outer(left, right):
    return lax.dot_general(
        left,
        right,
        (((0,), (0,)), ((), ())),
        precision=lax.Precision.HIGHEST,
        preferred_element_type=F32,
    )


def centre_kernel(x_ref, d_ref, a_ref, b_ref):
    rows, cols = x_ref.shape
    half = rows // 2
    mean = jnp.sum(x_ref[...], axis=0, keepdims=True) * (1.0 / rows)
    first, second = x_ref[0:half, :] - mean, x_ref[half:rows, :] - mean
    tail = jnp.broadcast_to(mean, (8, cols))
    d_ref[0:half, :] = first
    d_ref[half:rows, :] = second
    d_ref[rows : rows + 8, :] = tail
    a_ref[0:half, :] = first
    a_ref[half : half + 8, :] = tail
    b_ref[...] = second


def turn(piece, t_ref, at):
    cols = piece.shape[1]
    turned = piece.T
    high = turned.astype(BF16)
    t_ref[at : at + cols, :] = high
    t_ref[at + 2 * cols : at + 3 * cols, :] = (turned - high.astype(F32)).astype(BF16)


def against(t_ref, left, at, rows):
    high = left.astype(BF16)
    low = (left - high.astype(F32)).astype(BF16)
    two = t_ref.shape[0] // 2
    both = jnp.dot(t_ref[:, at : at + rows], high, preferred_element_type=F32)
    rest = jnp.dot(t_ref[0:two, at : at + rows], low, preferred_element_type=F32)
    return both[0:two] + (both[two:] + rest)


def deal(total, block, outs, at):
    cols = total.shape[1]
    y0, c = lax.axis_index("y0"), lax.axis_index("c")
    block[c] = total[0:cols].T.reshape(4, 2, 32, cols)
    block[1 - c] = total[cols:].T.reshape(4, 2, 32, cols)
    for dy in range(2):
        to = (1 - y0) if dy else y0
        for y1 in range(4):
            for j in range(2):
                lo = at + 32 * y1
                outs[dy][lo : lo + 32, cols * j : cols * j + cols] = block[j, y1, to]


def own_kernel(d_ref, s_ref, t_ref, *refs):
    outs, (block, mean) = refs[:2], refs[2:]
    cols = d_ref.shape[1]
    rows = d_ref.shape[0] - 8
    c = lax.axis_index("c")
    turn(d_ref[0:rows, :], t_ref, 0)
    turn(s_ref[0:rows, :], t_ref, cols)
    deal(against(t_ref, d_ref[0:rows, :], 0, rows), block, outs, 0)
    mean[c] = d_ref[rows : rows + 8, :]
    mean[1 - c] = s_ref[rows : rows + 8, :]
    for out in outs:
        out[128:136, :] = jnp.zeros((8, 2 * cols), F32)
        for j in range(2):
            out[128:129, cols * j : cols * j + cols] = mean[j, 0:1, :]
        out[129:130, 0:cols] = d_ref[rows : rows + 1, :]


def chips_kernel(n, t_ref, *refs):
    halves, outs, block = refs[: 2 * n], refs[2 * n : 2 * n + 2], refs[2 * n + 2]
    half, cols = halves[1].shape
    for k in range(n):
        a_ref, b_ref = halves[2 * k], halves[2 * k + 1]
        total = against(t_ref, a_ref[0:half, :], 0, half) + against(t_ref, b_ref[...], half, half)
        deal(total, block, outs, 128 * k)
    for out in outs:
        out[128 * n : 128 * n + 8, :] = jnp.zeros((8, 2 * cols), F32)
        for k in range(n):
            out[128 * n + k : 128 * n + k + 1, 0:cols] = halves[2 * k][half : half + 1, :]


def merge_pair_kernel(*refs):
    groups = [refs[3 * i : 3 * i + 3] for i in range(3)]
    keep_ref, send_ref, parts = refs[9:]
    cols = keep_ref.shape[1]
    z0, c = lax.axis_index("z0"), lax.axis_index("c")
    kept = jnp.full((1, 2 * cols), z0 == c)

    def read(group, lo, n):
        return jnp.where(kept, group[0][lo : lo + n, :], group[1][lo : lo + n, :]), group[2][lo : lo + n, :]

    def put(lo, value):
        n = value.shape[0]
        for j in range(2):
            parts[j, lo : lo + n, :] = value[:, cols * j : cols * j + cols]

    for group, n, at in zip(groups, (1, 2, 1), (0, 128, 384), strict=True):
        one, two = read(group, 0, 128 * n)
        put(at, one + two)
    put(512, jnp.zeros((16, 2 * cols), F32))
    own = read(groups[0], 128, 8)
    near = read(groups[1], 256, 8)
    far = read(groups[2], 128, 8)
    for dy in range(2):
        put(512 + dy, own[dy][0:1, :])
        for k, m in enumerate((own[dy][1:2, :], near[dy][0:1, :], near[dy][1:2, :], far[dy][0:1, :])):
            for j in range(2):
                parts[j, 514 + 2 * k + dy : 515 + 2 * k + dy, :] = m[:, 0:cols]
    keep_ref[...] = parts[c]
    send_ref[...] = parts[1 - c]


def merge_block_kernel(count, keep_ref, recv_ref, out_ref, shift):
    cols = keep_ref.shape[1]
    x, y0 = lax.axis_index("x"), lax.axis_index("y0")

    def centred(lo):
        means = jnp.concatenate([keep_ref[lo : lo + 2, :], recv_ref[lo : lo + 2, :]], axis=0)
        mean = jnp.sum(means, axis=0, keepdims=True) * 0.25
        return mean, jnp.concatenate([means - mean, jnp.zeros((4, cols), F32)], axis=0)

    own_mean, right = centred(512)
    for k, step in enumerate((0, 1, 3, 2)):
        mean, left = centred(514 + 2 * k)
        shift[...] = (outer(left, right) * float(count)).reshape(4, 2, 32, cols)
        to = lax.rem(x + step, 4)
        for y1 in range(4):
            lo = 128 * k + 32 * y1
            total = keep_ref[lo : lo + 32, :] + recv_ref[lo : lo + 32, :] + shift[y1, y0]
            out_ref[4 * to + y1, 0:32, :] = total
            out_ref[4 * to + y1, 32:33, :] = own_mean
            out_ref[4 * to + y1, 33:34, :] = mean
            out_ref[4 * to + y1, 34:40, :] = jnp.zeros((6, cols), F32)


def merge_all_kernel(count, in_ref, cov_ref, mean_ref, shift):
    blocks, _, cols = in_ref.shape
    total = in_ref[0, 0:32, :]
    for s in range(1, blocks):
        total = total + in_ref[s, 0:32, :]
    own = jnp.concatenate([in_ref[s, 32:33, :] for s in range(blocks)], axis=0)
    other = jnp.concatenate([in_ref[s, 33:34, :] for s in range(blocks)], axis=0)
    own_mean = jnp.sum(own, axis=0, keepdims=True) * (1.0 / blocks)
    other_mean = jnp.sum(other, axis=0, keepdims=True) * (1.0 / blocks)
    y = 2 * lax.axis_index("y1") + lax.axis_index("y0")
    shift[...] = (outer(other - other_mean, own - own_mean) * float(count)).reshape(8, 32, cols)
    cov_ref[...] = (total + shift[y]) / float(count * blocks - 1)
    mean_ref[...] = own_mean


def call(kernel, outs, args, scratch=(), mib=16, flops=0, moved=0):
    return pl.pallas_call(
        kernel,
        out_shape=outs,
        in_specs=[VMEM] * len(args),
        out_specs=jax.tree.map(lambda _: VMEM, outs),
        scratch_shapes=scratch,
        compiler_params=pltpu.CompilerParams(vmem_limit_bytes=mib * 2**20),
        cost_estimate=pl.CostEstimate(flops=flops, bytes_accessed=moved, transcendentals=0),
    )(*args)


def shifted(piece, axis, by):
    size = lax.axis_size(axis)
    return lax.ppermute(piece, axis, [(i, (i + by) % size) for i in range(size)])


def dealt(piece, dy):
    pairs = []
    for i in range(8):
        z0, y0, c = i // 4, i // 2 % 2, i % 2
        j = c * 4 + (y0 ^ dy) * 2 + z0
        if i != j:
            pairs.append((i, j))
    return lax.ppermute(piece, ("z0", "y0", "c"), pairs)


def steps(x):
    rows, cols = x.shape
    half = rows // 2
    d, a, b = call(
        centre_kernel,
        (shape(rows + 8, cols), shape(half + 8, cols), shape(half, cols)),
        (x,),
        flops=10**9,
        moved=2**21,
    )
    up_a = shifted(a, "x", -1)
    down_b = shifted(b, "x", 1)
    swap = shifted(d, "c", 1)
    block = pltpu.VMEM((2, 4, 2, 32, cols), F32)
    t, *own = call(
        own_kernel,
        (shape(4 * cols, rows, dtype=BF16), *[shape(136, 2 * cols)] * 2),
        (d, swap),
        (block, pltpu.VMEM((2, 8, cols), F32)),
        flops=2 * 10**9,
        moved=2**22,
    )
    a, b, *own = lax.optimization_barrier((a, b, *own))
    up_b = shifted(b, "x", -1)
    down_a = shifted(a, "x", 1)
    far_a = shifted(up_a, "x", -1)
    far_b = shifted(down_b, "x", 1)

    def gram(chips):
        n = len(chips) // 2
        return call(
            functools.partial(chips_kernel, n),
            [shape(128 * n + 8, 2 * cols)] * 2,
            (t, *chips),
            (block,),
            flops=2 * n * 10**9,
            moved=n * 2**21,
        )

    near = gram([up_a, up_b, down_a, down_b])
    far = gram([far_a, far_b])
    sums = []
    for outs in (own, near, far):
        sums += [outs[0]] + [dealt(outs[dy], dy) for dy in range(2)]
    keep, send = call(
        merge_pair_kernel,
        [shape(528, cols)] * 2,
        sums,
        (pltpu.VMEM((2, 528, cols), F32),),
        flops=10**9,
        moved=2**22,
    )
    merged = call(
        functools.partial(merge_block_kernel, rows),
        shape(16, 40, cols),
        (keep, shifted(send, "c", 1)),
        (pltpu.VMEM((4, 2, 32, cols), F32),),
        flops=10**9,
        moved=2**22,
    )
    merged = lax.all_to_all(merged, ("z1", "y1"), 0, 0, tiled=True)
    covariance, mean = call(
        functools.partial(merge_all_kernel, 4 * rows),
        (shape(32, cols), shape(1, cols)),
        (merged,),
        (pltpu.VMEM((8, 32, cols), F32),),
        flops=10**9,
        moved=2**20,
    )
    return covariance, mean.reshape(cols)


def solution(mesh):
    finer = Mesh(mesh.devices.reshape(4, 2, 4, 2, 4, 2), SCEN + FAC)
    return jax.shard_map(
        steps,
        mesh=finer,
        in_specs=(P(SCEN, FAC),),
        out_specs=(P(SCEN, FAC), P(FAC)),
        check_vma=False,
    )
```

```python
import functools

import jax
import jax.numpy as jnp
from jax import lax
from jax.experimental import pallas as pl
from jax.experimental.pallas import tpu as pltpu
from jax.sharding import Mesh
from jax.sharding import PartitionSpec as P


SCEN = ("z1", "z0", "y1", "y0")
FAC = ("x", "c")
VMEM = pl.BlockSpec(memory_space=pltpu.VMEM)
F32 = jnp.float32
BF16 = jnp.bfloat16


def shape(*dims, dtype=F32):
    return jax.ShapeDtypeStruct(dims, dtype)


def outer(left, right):
    return lax.dot_general(
        left,
        right,
        (((0,), (0,)), ((), ())),
        precision=lax.Precision.HIGHEST,
        preferred_element_type=F32,
    )


def centre_kernel(x_ref, d_ref):
    rows, cols = x_ref.shape
    mean = jnp.sum(x_ref[...], axis=0, keepdims=True) * (1.0 / rows)
    d_ref[0:rows, :] = x_ref[...] - mean
    d_ref[rows : rows + 8, :] = jnp.broadcast_to(mean, (8, cols))


def turn(piece, t_ref, at):
    cols = piece.shape[1]
    high, low = split(piece.T)
    t_ref[at : at + cols, :] = high
    t_ref[at + 2 * cols : at + 3 * cols, :] = low


def split(value):
    high = value.astype(BF16)
    return high, (value - high.astype(F32)).astype(BF16)


def against(t_ref, left):
    high, low = split(left)
    two = t_ref.shape[0] // 2
    both = jnp.dot(t_ref[...], high, preferred_element_type=F32)
    rest = jnp.dot(t_ref[0:two, :], low, preferred_element_type=F32)
    return both[0:two] + (both[two:] + rest)


def deal(total, block, outs, at):
    cols = total.shape[1]
    y0, c = lax.axis_index("y0"), lax.axis_index("c")
    block[c] = total[0:cols].T.reshape(4, 2, 32, cols)
    block[1 - c] = total[cols:].T.reshape(4, 2, 32, cols)
    for dy in range(2):
        to = (1 - y0) if dy else y0
        for y1 in range(4):
            for j in range(2):
                lo = at + 32 * y1
                outs[dy][lo : lo + 32, cols * j : cols * j + cols] = block[j, y1, to]


def own_kernel(d_ref, s_ref, t_ref, *refs):
    outs, (block, mean) = refs[:2], refs[2:]
    cols = d_ref.shape[1]
    rows = d_ref.shape[0] - 8
    c = lax.axis_index("c")
    turn(d_ref[0:rows, :], t_ref, 0)
    turn(s_ref[0:rows, :], t_ref, cols)
    deal(against(t_ref, d_ref[0:rows, :]), block, outs, 0)
    mean[c] = d_ref[rows : rows + 8, :]
    mean[1 - c] = s_ref[rows : rows + 8, :]
    for out in outs:
        out[128:136, :] = jnp.zeros((8, 2 * cols), F32)
        for j in range(2):
            out[128:129, cols * j : cols * j + cols] = mean[j, 0:1, :]
        out[129:130, 0:cols] = d_ref[rows : rows + 1, :]


def near_kernel(t_ref, up_ref, down_ref, *refs):
    outs, block = refs[:2], refs[2]
    rows, cols = up_ref.shape[0] - 8, up_ref.shape[1]
    for k, ref in enumerate((up_ref, down_ref)):
        deal(against(t_ref, ref[0:rows, :]), block, outs, 128 * k)
    for out in outs:
        out[256:264, :] = jnp.zeros((8, 2 * cols), F32)
        for k, ref in enumerate((up_ref, down_ref)):
            out[256 + k : 257 + k, 0:cols] = ref[rows : rows + 1, :]


def far_kernel(up_ref, down_ref, cross_ref, *refs):
    outs, (block, mean) = refs[:4], refs[4:]
    rows, cols = up_ref.shape[0] - 8, up_ref.shape[1]
    z0, y0 = lax.axis_index("z0"), lax.axis_index("y0")
    crossed = jnp.full((1, cols), lax.axis_index("x") >= 2)
    other = jnp.where(crossed, cross_ref[...], down_ref[...])
    high, low = split(up_ref[0:rows, :].T)
    right_high, right_low = split(other[0:rows])
    product = jnp.dot(high, right_high, preferred_element_type=F32) + (
        jnp.dot(low, right_high, preferred_element_type=F32) + jnp.dot(high, right_low, preferred_element_type=F32)
    )
    block[0] = product.reshape(4, 2, 32, cols)
    block[1] = product.T.reshape(4, 2, 32, cols)
    mean[0] = up_ref[rows : rows + 8, :]
    mean[1] = other[rows : rows + 8]
    for p, out in enumerate(outs):
        dy, s = divmod(p, 2)
        kind = (1 - z0) if s else z0
        to = (1 - y0) if dy else y0
        for y1 in range(4):
            out[32 * y1 : 32 * y1 + 32, :] = block[kind, y1, to]
        out[128:129, :] = mean[kind, 0:1, :]
        out[129:130, :] = mean[1 - kind, 0:1, :]
        out[130:136, :] = jnp.zeros((6, cols), F32)


def merge_pair_kernel(*refs):
    groups = (refs[0:3], refs[3:6])
    keep_ref, send_ref, parts = refs[6:]
    cols = keep_ref.shape[1]
    z0, c = lax.axis_index("z0"), lax.axis_index("c")
    kept = jnp.full((1, 2 * cols), z0 == c)

    def read(group, lo, n):
        return jnp.where(kept, group[0][lo : lo + n, :], group[1][lo : lo + n, :]), group[2][lo : lo + n, :]

    def put(lo, value):
        n = value.shape[0]
        for j in range(2):
            parts[j, lo : lo + n, :] = value[:, cols * j : cols * j + cols]

    for group, n, at in zip(groups, (1, 2), (0, 128), strict=True):
        one, two = read(group, 0, 128 * n)
        put(at, one + two)
    own = read(groups[0], 128, 8)
    near = read(groups[1], 256, 8)
    for dy in range(2):
        put(384 + dy, own[dy][0:1, :])
        for k, m in enumerate((own[dy][1:2, :], near[dy][0:1, :], near[dy][1:2, :])):
            for j in range(2):
                parts[j, 386 + 2 * k + dy : 387 + 2 * k + dy, :] = m[:, 0:cols]
    keep_ref[...] = parts[c]
    send_ref[...] = parts[1 - c]


def merge_block_kernel(count, keep_ref, recv_ref, *refs):
    far, (out_ref, shift) = refs[:4], refs[4:]
    cols = keep_ref.shape[1]
    x, y0 = lax.axis_index("x"), lax.axis_index("y0")
    zeros = jnp.zeros((4, cols), F32)

    def mean_of(means):
        return jnp.sum(means, axis=0, keepdims=True) * 0.25

    def pairs(lo):
        return jnp.concatenate([keep_ref[lo : lo + 2, :], recv_ref[lo : lo + 2, :]], axis=0)

    own_means = pairs(384)
    own_mean = mean_of(own_means)
    for k, step in enumerate((0, 1, 3, 2)):
        if k < 3:
            means, right = pairs(386 + 2 * k), own_means
        else:
            means = jnp.concatenate([f[128:129, :] for f in far], axis=0)
            right = jnp.concatenate([f[129:130, :] for f in far], axis=0)
        mean = mean_of(means)
        left = jnp.concatenate([means - mean, zeros], axis=0)
        right = jnp.concatenate([right - own_mean, zeros], axis=0)
        shift[...] = (outer(left, right) * float(count)).reshape(4, 2, 32, cols)
        to = lax.rem(x + step, 4)
        for y1 in range(4):
            if k < 3:
                lo = 128 * k + 32 * y1
                total = keep_ref[lo : lo + 32, :] + recv_ref[lo : lo + 32, :]
            else:
                lo = 32 * y1
                total = (far[0][lo : lo + 32, :] + far[1][lo : lo + 32, :]) + (
                    far[2][lo : lo + 32, :] + far[3][lo : lo + 32, :]
                )
            out_ref[4 * to + y1, 0:32, :] = total + shift[y1, y0]
            out_ref[4 * to + y1, 32:33, :] = own_mean
            out_ref[4 * to + y1, 33:34, :] = mean
            out_ref[4 * to + y1, 34:40, :] = jnp.zeros((6, cols), F32)


def merge_all_kernel(count, in_ref, cov_ref, mean_ref, shift):
    blocks, _, cols = in_ref.shape
    total = in_ref[0, 0:32, :]
    for s in range(1, blocks):
        total = total + in_ref[s, 0:32, :]
    own = jnp.concatenate([in_ref[s, 32:33, :] for s in range(blocks)], axis=0)
    other = jnp.concatenate([in_ref[s, 33:34, :] for s in range(blocks)], axis=0)
    own_mean = jnp.sum(own, axis=0, keepdims=True) * (1.0 / blocks)
    other_mean = jnp.sum(other, axis=0, keepdims=True) * (1.0 / blocks)
    y = 2 * lax.axis_index("y1") + lax.axis_index("y0")
    shift[...] = (outer(other - other_mean, own - own_mean) * float(count)).reshape(8, 32, cols)
    cov_ref[...] = (total + shift[y]) / float(count * blocks - 1)
    mean_ref[...] = own_mean


def call(kernel, outs, args, scratch=(), mib=16, flops=0, moved=0):
    return pl.pallas_call(
        kernel,
        out_shape=outs,
        in_specs=[VMEM] * len(args),
        out_specs=jax.tree.map(lambda _: VMEM, outs),
        scratch_shapes=scratch,
        compiler_params=pltpu.CompilerParams(vmem_limit_bytes=mib * 2**20),
        cost_estimate=pl.CostEstimate(flops=flops, bytes_accessed=moved, transcendentals=0),
    )(*args)


def shifted(piece, axis, by):
    size = lax.axis_size(axis)
    return lax.ppermute(piece, axis, [(i, (i + by) % size) for i in range(size)])


def dealt(piece, dy):
    pairs = []
    for i in range(8):
        z0, y0, c = i // 4, i // 2 % 2, i % 2
        j = c * 4 + (y0 ^ dy) * 2 + z0
        if i != j:
            pairs.append((i, j))
    return lax.ppermute(piece, ("z0", "y0", "c"), pairs)


def between(piece, dy, s):
    pairs = []
    for i in range(32):
        z0, y0, x, c = i // 16, i // 8 % 2, i // 2 % 4, i % 2
        j = 1 - c if x >= 2 else c
        x_to, z_to, c_to = ((x + 1) % 4, j, c) if z0 ^ s else ((x + 3) % 4, c, j)
        pairs.append((i, z_to * 16 + (y0 ^ dy) * 8 + x_to * 2 + c_to))
    return lax.ppermute(piece, ("z0", "y0", "x", "c"), pairs)


def crossed(piece):
    return lax.ppermute(piece, ("x", "c"), [(4, 5), (5, 4), (6, 7), (7, 6)])


def steps(x):
    rows, cols = x.shape
    d = call(centre_kernel, shape(rows + 8, cols), (x,), flops=10**9, moved=2**21)
    up = shifted(d, "x", -1)
    down = shifted(d, "x", 1)
    swap = shifted(d, "c", 1)
    block = pltpu.VMEM((2, 4, 2, 32, cols), F32)
    mean = pltpu.VMEM((2, 8, cols), F32)
    t, *own = call(
        own_kernel,
        (shape(4 * cols, rows, dtype=BF16), *[shape(136, 2 * cols)] * 2),
        (d, swap),
        (block, mean),
        flops=2 * 10**9,
        moved=2**22,
    )
    near = call(near_kernel, [shape(264, 2 * cols)] * 2, (t, up, down), (block,), flops=4 * 10**9, moved=2**22)
    cross = crossed(down)
    far = call(far_kernel, [shape(136, cols)] * 4, (up, down, cross), (block, mean), flops=10**9, moved=2**22)
    far = [between(far[p], *divmod(p, 2)) for p in range(4)]
    sums = []
    for outs in (own, near):
        sums += [outs[0]] + [dealt(outs[dy], dy) for dy in range(2)]
    keep, send = call(
        merge_pair_kernel,
        [shape(392, cols)] * 2,
        sums,
        (pltpu.VMEM((2, 392, cols), F32),),
        flops=10**9,
        moved=2**22,
    )
    recv = shifted(send, "c", 1)
    merged = call(
        functools.partial(merge_block_kernel, rows),
        shape(16, 40, cols),
        (keep, recv, *far),
        (pltpu.VMEM((4, 2, 32, cols), F32),),
        flops=10**9,
        moved=2**22,
    )
    merged = lax.all_to_all(merged, ("z1", "y1"), 0, 0, tiled=True)
    covariance, mean = call(
        functools.partial(merge_all_kernel, 4 * rows),
        (shape(32, cols), shape(1, cols)),
        (merged,),
        (pltpu.VMEM((8, 32, cols), F32),),
        flops=10**9,
        moved=2**20,
    )
    return covariance, mean.reshape(cols)


def solution(mesh):
    finer = Mesh(mesh.devices.reshape(4, 2, 4, 2, 4, 2), SCEN + FAC)
    return jax.shard_map(
        steps,
        mesh=finer,
        in_specs=(P(SCEN, FAC),),
        out_specs=(P(SCEN, FAC), P(FAC)),
        check_vma=False,
    )
```

```python
import functools

import jax
import jax.numpy as jnp
from jax import lax
from jax.experimental import pallas as pl
from jax.experimental.pallas import tpu as pltpu
from jax.sharding import Mesh
from jax.sharding import PartitionSpec as P


SCEN = ("z1", "z0", "y1", "y0")
FAC = ("x", "c")
VMEM = pl.BlockSpec(memory_space=pltpu.VMEM)
F32 = jnp.float32
BF16 = jnp.bfloat16


def shape(*dims, dtype=F32):
    return jax.ShapeDtypeStruct(dims, dtype)


def outer(left, right):
    return lax.dot_general(
        left,
        right,
        (((0,), (0,)), ((), ())),
        precision=lax.Precision.HIGHEST,
        preferred_element_type=F32,
    )


def centre_kernel(x_ref, d_ref):
    rows, cols = x_ref.shape
    mean = jnp.sum(x_ref[...], axis=0, keepdims=True) * (1.0 / rows)
    d_ref[0:rows, :] = x_ref[...] - mean
    d_ref[rows : rows + 8, :] = jnp.broadcast_to(mean, (8, cols))


def turn(piece, t_ref, at):
    cols = piece.shape[1]
    high, low = split(piece.T)
    t_ref[at : at + cols, :] = high
    t_ref[at + 2 * cols : at + 3 * cols, :] = low


def split(value):
    high = value.astype(BF16)
    return high, (value - high.astype(F32)).astype(BF16)


def against(t_ref, left):
    high, low = split(left)
    two = t_ref.shape[0] // 2
    both = jnp.dot(t_ref[...], high, preferred_element_type=F32)
    rest = jnp.dot(t_ref[0:two, :], low, preferred_element_type=F32)
    return both[0:two] + (both[two:] + rest)


def deal(total, block, outs, at):
    cols = total.shape[1]
    y0, c = lax.axis_index("y0"), lax.axis_index("c")
    block[c] = total[0:cols].T.reshape(4, 2, 32, cols)
    block[1 - c] = total[cols:].T.reshape(4, 2, 32, cols)
    for dy in range(2):
        to = (1 - y0) if dy else y0
        for y1 in range(4):
            for j in range(2):
                lo = at + 32 * y1
                outs[dy][lo : lo + 32, cols * j : cols * j + cols] = block[j, y1, to]


def own_kernel(d_ref, s_ref, t_ref, *refs):
    outs, (block, mean) = refs[:2], refs[2:]
    cols = d_ref.shape[1]
    rows = d_ref.shape[0] - 8
    c = lax.axis_index("c")
    turn(d_ref[0:rows, :], t_ref, 0)
    turn(s_ref[0:rows, :], t_ref, cols)
    deal(against(t_ref, d_ref[0:rows, :]), block, outs, 0)
    mean[c] = d_ref[rows : rows + 8, :]
    mean[1 - c] = s_ref[rows : rows + 8, :]
    for out in outs:
        out[128:136, :] = jnp.zeros((8, 2 * cols), F32)
        for j in range(2):
            out[128:129, cols * j : cols * j + cols] = mean[j, 0:1, :]
        out[129:130, 0:cols] = d_ref[rows : rows + 1, :]


def above_kernel(t_ref, up_ref, *refs):
    outs, block = refs[:2], refs[2]
    rows = up_ref.shape[0] - 8
    deal(against(t_ref, up_ref[0:rows, :]), block, outs, 0)


def near_kernel(t_ref, up_ref, down_ref, *refs):
    above, outs, block = refs[:2], refs[2:4], refs[4]
    rows, cols = up_ref.shape[0] - 8, up_ref.shape[1]
    deal(against(t_ref, down_ref[0:rows, :]), block, outs, 128)
    for part, out in zip(above, outs, strict=True):
        out[0:128, :] = part[...]
        out[256:264, :] = jnp.zeros((8, 2 * cols), F32)
        for k, ref in enumerate((up_ref, down_ref)):
            out[256 + k : 257 + k, 0:cols] = ref[rows : rows + 1, :]


def far_kernel(up_ref, down_ref, cross_ref, *refs):
    outs, (block, mean) = refs[:4], refs[4:]
    rows, cols = up_ref.shape[0] - 8, up_ref.shape[1]
    z0, y0 = lax.axis_index("z0"), lax.axis_index("y0")
    crossed = jnp.full((1, cols), lax.axis_index("x") >= 2)
    above = jnp.where(crossed, cross_ref[...], up_ref[...])
    high, low = split(above[0:rows].T)
    right_high, right_low = split(down_ref[0:rows, :])
    product = jnp.dot(high, right_high, preferred_element_type=F32) + (
        jnp.dot(low, right_high, preferred_element_type=F32) + jnp.dot(high, right_low, preferred_element_type=F32)
    )
    block[0] = product.reshape(4, 2, 32, cols)
    block[1] = product.T.reshape(4, 2, 32, cols)
    mean[0] = above[rows : rows + 8]
    mean[1] = down_ref[rows : rows + 8, :]
    for p, out in enumerate(outs):
        dy, s = divmod(p, 2)
        kind = (1 - z0) if s else z0
        to = (1 - y0) if dy else y0
        for y1 in range(4):
            out[32 * y1 : 32 * y1 + 32, :] = block[kind, y1, to]
        out[128:129, :] = mean[kind, 0:1, :]
        out[129:130, :] = mean[1 - kind, 0:1, :]
        out[130:136, :] = jnp.zeros((6, cols), F32)


def merge_pair_kernel(*refs):
    groups = (refs[0:3], refs[3:6])
    keep_ref, send_ref, parts = refs[6:]
    cols = keep_ref.shape[1]
    z0, c = lax.axis_index("z0"), lax.axis_index("c")
    kept = jnp.full((1, 2 * cols), z0 == c)

    def read(group, lo, n):
        return jnp.where(kept, group[0][lo : lo + n, :], group[1][lo : lo + n, :]), group[2][lo : lo + n, :]

    def put(lo, value):
        n = value.shape[0]
        for j in range(2):
            parts[j, lo : lo + n, :] = value[:, cols * j : cols * j + cols]

    for group, n, at in zip(groups, (1, 2), (0, 128), strict=True):
        one, two = read(group, 0, 128 * n)
        put(at, one + two)
    own = read(groups[0], 128, 8)
    near = read(groups[1], 256, 8)
    for dy in range(2):
        put(384 + dy, own[dy][0:1, :])
        for k, m in enumerate((own[dy][1:2, :], near[dy][0:1, :], near[dy][1:2, :])):
            for j in range(2):
                parts[j, 386 + 2 * k + dy : 387 + 2 * k + dy, :] = m[:, 0:cols]
    keep_ref[...] = parts[c]
    send_ref[...] = parts[1 - c]


def merge_block_kernel(count, keep_ref, recv_ref, *refs):
    far, (out_ref, shift) = refs[:4], refs[4:]
    cols = keep_ref.shape[1]
    x, y0 = lax.axis_index("x"), lax.axis_index("y0")
    zeros = jnp.zeros((4, cols), F32)

    def mean_of(means):
        return jnp.sum(means, axis=0, keepdims=True) * 0.25

    def pairs(lo):
        return jnp.concatenate([keep_ref[lo : lo + 2, :], recv_ref[lo : lo + 2, :]], axis=0)

    own_means = pairs(384)
    own_mean = mean_of(own_means)
    far_means = jnp.concatenate([f[129:130, :] for f in far], axis=0)
    right = jnp.concatenate([own_means - own_mean, far_means - own_mean], axis=0)
    row_means, left = [], []
    for k in range(4):
        means = pairs(386 + 2 * k) if k < 3 else jnp.concatenate([f[128:129, :] for f in far], axis=0)
        mean = mean_of(means)
        row_means.append(mean)
        left.append(jnp.concatenate([means - mean, zeros] if k < 3 else [zeros, means - mean], axis=0))
    moved = outer(jnp.concatenate(left, axis=1), right) * float(count)
    shift[...] = moved.reshape(4, 4, 2, 32, cols)
    for k, step in enumerate((0, 1, 3, 2)):
        to = lax.rem(x + step, 4)
        for y1 in range(4):
            if k < 3:
                lo = 128 * k + 32 * y1
                total = keep_ref[lo : lo + 32, :] + recv_ref[lo : lo + 32, :]
            else:
                lo = 32 * y1
                total = (far[0][lo : lo + 32, :] + far[1][lo : lo + 32, :]) + (
                    far[2][lo : lo + 32, :] + far[3][lo : lo + 32, :]
                )
            out_ref[4 * to + y1, 0:32, :] = total + shift[k, y1, y0]
            out_ref[4 * to + y1, 32:33, :] = own_mean
            out_ref[4 * to + y1, 33:34, :] = row_means[k]
            out_ref[4 * to + y1, 34:40, :] = jnp.zeros((6, cols), F32)


def merge_all_kernel(count, in_ref, cov_ref, mean_ref, shift):
    blocks, _, cols = in_ref.shape
    total = in_ref[0, 0:32, :]
    for s in range(1, blocks):
        total = total + in_ref[s, 0:32, :]
    own = jnp.concatenate([in_ref[s, 32:33, :] for s in range(blocks)], axis=0)
    other = jnp.concatenate([in_ref[s, 33:34, :] for s in range(blocks)], axis=0)
    own_mean = jnp.sum(own, axis=0, keepdims=True) * (1.0 / blocks)
    other_mean = jnp.sum(other, axis=0, keepdims=True) * (1.0 / blocks)
    y = 2 * lax.axis_index("y1") + lax.axis_index("y0")
    shift[...] = (outer(other - other_mean, own - own_mean) * float(count)).reshape(8, 32, cols)
    cov_ref[...] = (total + shift[y]) / float(count * blocks - 1)
    mean_ref[...] = own_mean


def call(kernel, outs, args, scratch=(), mib=16, flops=0, moved=0):
    return pl.pallas_call(
        kernel,
        out_shape=outs,
        in_specs=[VMEM] * len(args),
        out_specs=jax.tree.map(lambda _: VMEM, outs),
        scratch_shapes=scratch,
        compiler_params=pltpu.CompilerParams(vmem_limit_bytes=mib * 2**20),
        cost_estimate=pl.CostEstimate(flops=flops, bytes_accessed=moved, transcendentals=0),
    )(*args)


def shifted(piece, axis, by):
    size = lax.axis_size(axis)
    return lax.ppermute(piece, axis, [(i, (i + by) % size) for i in range(size)])


def dealt(piece, dy):
    pairs = []
    for i in range(8):
        z0, y0, c = i // 4, i // 2 % 2, i % 2
        j = c * 4 + (y0 ^ dy) * 2 + z0
        if i != j:
            pairs.append((i, j))
    return lax.ppermute(piece, ("z0", "y0", "c"), pairs)


def between(piece, dy, s):
    pairs = []
    for i in range(32):
        z0, y0, x, c = i // 16, i // 8 % 2, i // 2 % 4, i % 2
        above = 1 - c if x >= 2 else c
        x_to, z_to, c_to = ((x + 1) % 4, c, above) if z0 ^ s else ((x + 3) % 4, above, c)
        pairs.append((i, z_to * 16 + (y0 ^ dy) * 8 + x_to * 2 + c_to))
    return lax.ppermute(piece, ("z0", "y0", "x", "c"), pairs)


def crossed(piece):
    return lax.ppermute(piece, ("x", "c"), [(4, 5), (5, 4), (6, 7), (7, 6)])


def steps(x):
    rows, cols = x.shape
    d = call(centre_kernel, shape(rows + 8, cols), (x,), flops=10**9, moved=2**21)
    up = shifted(d, "x", -1)
    down = shifted(d, "x", 1)
    swap = shifted(d, "c", 1)
    block = pltpu.VMEM((2, 4, 2, 32, cols), F32)
    mean = pltpu.VMEM((2, 8, cols), F32)
    t, *own = call(
        own_kernel,
        (shape(4 * cols, rows, dtype=BF16), *[shape(136, 2 * cols)] * 2),
        (d, swap),
        (block, mean),
        flops=2 * 10**9,
        moved=2**22,
    )
    cross = crossed(up)
    above = call(above_kernel, [shape(128, 2 * cols)] * 2, (t, up), (block,), flops=2 * 10**9, moved=2**22)
    near = call(near_kernel, [shape(264, 2 * cols)] * 2, (t, up, down, *above), (block,), flops=2 * 10**9, moved=2**22)
    far = call(far_kernel, [shape(136, cols)] * 4, (up, down, cross), (block, mean), flops=10**9, moved=2**22)
    far = [between(far[p], *divmod(p, 2)) for p in range(4)]
    sums = []
    for outs in (own, near):
        sums += [outs[0]] + [dealt(outs[dy], dy) for dy in range(2)]
    keep, send = call(
        merge_pair_kernel,
        [shape(392, cols)] * 2,
        sums,
        (pltpu.VMEM((2, 392, cols), F32),),
        flops=10**9,
        moved=2**22,
    )
    recv = shifted(send, "c", 1)
    merged = call(
        functools.partial(merge_block_kernel, rows),
        shape(16, 40, cols),
        (keep, recv, *far),
        (pltpu.VMEM((4, 4, 2, 32, cols), F32),),
        flops=10**9,
        moved=2**22,
    )
    merged = lax.all_to_all(merged, ("z1", "y1"), 0, 0, tiled=True)
    covariance, mean = call(
        functools.partial(merge_all_kernel, 4 * rows),
        (shape(32, cols), shape(1, cols)),
        (merged,),
        (pltpu.VMEM((8, 32, cols), F32),),
        flops=10**9,
        moved=2**20,
    )
    return covariance, mean.reshape(cols)


def solution(mesh):
    finer = Mesh(mesh.devices.reshape(4, 2, 4, 2, 4, 2), SCEN + FAC)
    return jax.shard_map(
        steps,
        mesh=finer,
        in_specs=(P(SCEN, FAC),),
        out_specs=(P(SCEN, FAC), P(FAC)),
        check_vma=False,
    )
```

```python
import functools

import jax
import jax.numpy as jnp
from jax import lax
from jax.experimental import pallas as pl
from jax.experimental.pallas import tpu as pltpu
from jax.sharding import Mesh
from jax.sharding import PartitionSpec as P


SCEN = ("z1", "z0", "y1", "y0")
FAC = ("x", "c")
VMEM = pl.BlockSpec(memory_space=pltpu.VMEM)
F32 = jnp.float32
BF16 = jnp.bfloat16


def shape(*dims, dtype=F32):
    return jax.ShapeDtypeStruct(dims, dtype)


def split(value):
    high = value.astype(BF16)
    return high, (value - high.astype(F32)).astype(BF16)


def outer(left, right):
    def product(one, two):
        return lax.dot_general(one, two, (((0,), (0,)), ((), ())), preferred_element_type=F32)

    left_high, left_low = split(left)
    right_high, right_low = split(right)
    return product(left_high, right_high) + (product(left_low, right_high) + product(left_high, right_low))


def centre_kernel(x_ref, d_ref):
    rows, cols = x_ref.shape
    mean = jnp.sum(x_ref[...], axis=0, keepdims=True) * (1.0 / rows)
    d_ref[0:rows, :] = x_ref[...] - mean
    d_ref[rows : rows + 8, :] = jnp.broadcast_to(mean, (8, cols))


def turn(piece, t_ref, at):
    cols = piece.shape[1]
    high, low = split(piece.T)
    t_ref[at : at + cols, :] = high
    t_ref[at + 2 * cols : at + 3 * cols, :] = low


def against(t_ref, left):
    high, low = split(left)
    two = t_ref.shape[0] // 2
    both = jnp.dot(t_ref[...], high, preferred_element_type=F32)
    rest = jnp.dot(t_ref[0:two, :], low, preferred_element_type=F32)
    return both[0:two] + (both[two:] + rest)


def deal(total, block, outs, at):
    cols = total.shape[1]
    y0, c = lax.axis_index("y0"), lax.axis_index("c")
    block[c] = total[0:cols].T.reshape(4, 2, 32, cols)
    block[1 - c] = total[cols:].T.reshape(4, 2, 32, cols)
    for dy in range(2):
        to = (1 - y0) if dy else y0
        for y1 in range(4):
            for j in range(2):
                lo = at + 32 * y1
                outs[dy][lo : lo + 32, cols * j : cols * j + cols] = block[j, y1, to]


def own_kernel(d_ref, s_ref, t_ref, *refs):
    outs, (block, mean) = refs[:2], refs[2:]
    cols = d_ref.shape[1]
    rows = d_ref.shape[0] - 8
    c = lax.axis_index("c")
    turn(d_ref[0:rows, :], t_ref, 0)
    turn(s_ref[0:rows, :], t_ref, cols)
    deal(against(t_ref, d_ref[0:rows, :]), block, outs, 0)
    mean[c] = d_ref[rows : rows + 8, :]
    mean[1 - c] = s_ref[rows : rows + 8, :]
    for out in outs:
        out[128:136, :] = jnp.zeros((8, 2 * cols), F32)
        for j in range(2):
            out[128:129, cols * j : cols * j + cols] = mean[j, 0:1, :]
        out[129:130, 0:cols] = d_ref[rows : rows + 1, :]


def above_kernel(t_ref, up_ref, *refs):
    outs, block = refs[:2], refs[2]
    rows = up_ref.shape[0] - 8
    deal(against(t_ref, up_ref[0:rows, :]), block, outs, 0)


def near_kernel(t_ref, up_ref, down_ref, *refs):
    above, outs, block = refs[:2], refs[2:4], refs[4]
    rows, cols = up_ref.shape[0] - 8, up_ref.shape[1]
    deal(against(t_ref, down_ref[0:rows, :]), block, outs, 128)
    for part, out in zip(above, outs, strict=True):
        out[0:128, :] = part[...]
        out[256:264, :] = jnp.zeros((8, 2 * cols), F32)
        for k, ref in enumerate((up_ref, down_ref)):
            out[256 + k : 257 + k, 0:cols] = ref[rows : rows + 1, :]


def far_kernel(up_ref, down_ref, cross_ref, *refs):
    outs, (block, mean) = refs[:4], refs[4:]
    rows, cols = up_ref.shape[0] - 8, up_ref.shape[1]
    z0, y0 = lax.axis_index("z0"), lax.axis_index("y0")
    crossed = jnp.full((1, cols), lax.axis_index("x") >= 2)
    above = jnp.where(crossed, cross_ref[...], up_ref[...])
    high, low = split(above[0:rows].T)
    right_high, right_low = split(down_ref[0:rows, :])
    product = jnp.dot(high, right_high, preferred_element_type=F32) + (
        jnp.dot(low, right_high, preferred_element_type=F32) + jnp.dot(high, right_low, preferred_element_type=F32)
    )
    block[0] = product.reshape(4, 2, 32, cols)
    block[1] = product.T.reshape(4, 2, 32, cols)
    mean[0] = above[rows : rows + 8]
    mean[1] = down_ref[rows : rows + 8, :]
    for p, out in enumerate(outs):
        dy, s = divmod(p, 2)
        kind = (1 - z0) if s else z0
        to = (1 - y0) if dy else y0
        for y1 in range(4):
            out[32 * y1 : 32 * y1 + 32, :] = block[kind, y1, to]
        out[128:129, :] = mean[kind, 0:1, :]
        out[129:130, :] = mean[1 - kind, 0:1, :]
        out[130:136, :] = jnp.zeros((6, cols), F32)


def merge_pair_kernel(*refs):
    groups = (refs[0:3], refs[3:6])
    keep_ref, send_ref, parts = refs[6:]
    cols = keep_ref.shape[1]
    z0, c = lax.axis_index("z0"), lax.axis_index("c")
    kept = jnp.full((1, 2 * cols), z0 == c)

    def read(group, lo, n):
        return jnp.where(kept, group[0][lo : lo + n, :], group[1][lo : lo + n, :]), group[2][lo : lo + n, :]

    def put(lo, value):
        n = value.shape[0]
        for j in range(2):
            parts[j, lo : lo + n, :] = value[:, cols * j : cols * j + cols]

    for group, n, at in zip(groups, (1, 2), (0, 128), strict=True):
        one, two = read(group, 0, 128 * n)
        put(at, one + two)
    own = read(groups[0], 128, 8)
    near = read(groups[1], 256, 8)
    for dy in range(2):
        put(384 + dy, own[dy][0:1, :])
        for k, m in enumerate((own[dy][1:2, :], near[dy][0:1, :], near[dy][1:2, :])):
            for j in range(2):
                parts[j, 386 + 2 * k + dy : 387 + 2 * k + dy, :] = m[:, 0:cols]
    keep_ref[...] = parts[c]
    send_ref[...] = parts[1 - c]


def merge_block_kernel(count, keep_ref, recv_ref, *refs):
    far, (out_ref, shift) = refs[:4], refs[4:]
    cols = keep_ref.shape[1]
    x, y0 = lax.axis_index("x"), lax.axis_index("y0")
    zeros = jnp.zeros((4, cols), F32)

    def mean_of(means):
        return jnp.sum(means, axis=0, keepdims=True) * 0.25

    def pairs(lo):
        return jnp.concatenate([keep_ref[lo : lo + 2, :], recv_ref[lo : lo + 2, :]], axis=0)

    own_means = pairs(384)
    own_mean = mean_of(own_means)
    far_means = jnp.concatenate([f[129:130, :] for f in far], axis=0)
    right = jnp.concatenate([own_means - own_mean, far_means - own_mean], axis=0)
    row_means, left = [], []
    for k in range(4):
        means = pairs(386 + 2 * k) if k < 3 else jnp.concatenate([f[128:129, :] for f in far], axis=0)
        mean = mean_of(means)
        row_means.append(mean)
        left.append(jnp.concatenate([means - mean, zeros] if k < 3 else [zeros, means - mean], axis=0))
    moved = outer(jnp.concatenate(left, axis=1), right) * float(count)
    shift[...] = moved.reshape(4, 4, 2, 32, cols)
    for k, step in enumerate((0, 1, 3, 2)):
        to = lax.rem(x + step, 4)
        for y1 in range(4):
            if k < 3:
                lo = 128 * k + 32 * y1
                total = keep_ref[lo : lo + 32, :] + recv_ref[lo : lo + 32, :]
            else:
                lo = 32 * y1
                total = (far[0][lo : lo + 32, :] + far[1][lo : lo + 32, :]) + (
                    far[2][lo : lo + 32, :] + far[3][lo : lo + 32, :]
                )
            total = total + shift[k, y1, y0]
            for g in range(4):
                out_ref[4 * to + y1, :, cols * g : cols * g + cols] = total[8 * g : 8 * g + 8, :]
            for row, m in ((0, own_mean), (2, row_means[k])):
                for h in range(2):
                    out_ref[4 * to + y1, row + h : row + h + 1, 4 * cols :] = m[:, 128 * h : 128 * h + 128]
            out_ref[4 * to + y1, 4:8, 4 * cols :] = jnp.zeros((4, 128), F32)


def merge_all_kernel(count, in_ref, cov_ref, mean_ref, shift):
    blocks = in_ref.shape[0]
    cols = cov_ref.shape[1]
    total = in_ref[0]
    for s in range(1, blocks):
        total = total + in_ref[s]

    def means(row):
        halves = [
            jnp.concatenate([in_ref[s, row + h : row + h + 1, 4 * cols :] for s in range(blocks)], axis=0)
            for h in range(2)
        ]
        return jnp.concatenate(halves, axis=1)

    own, other = means(0), means(2)
    own_mean = jnp.sum(own, axis=0, keepdims=True) * (1.0 / blocks)
    other_mean = jnp.sum(other, axis=0, keepdims=True) * (1.0 / blocks)
    y = 2 * lax.axis_index("y1") + lax.axis_index("y0")
    shift[...] = (outer(other - other_mean, own - own_mean) * float(count)).reshape(8, 4, 8, cols)
    for g in range(4):
        here = total[:, cols * g : cols * g + cols] + shift[y, g]
        cov_ref[8 * g : 8 * g + 8, :] = here / float(count * blocks - 1)
    mean_ref[...] = own_mean


def call(kernel, outs, args, scratch=(), mib=16, flops=0, moved=0):
    return pl.pallas_call(
        kernel,
        out_shape=outs,
        in_specs=[VMEM] * len(args),
        out_specs=jax.tree.map(lambda _: VMEM, outs),
        scratch_shapes=scratch,
        compiler_params=pltpu.CompilerParams(vmem_limit_bytes=mib * 2**20),
        cost_estimate=pl.CostEstimate(flops=flops, bytes_accessed=moved, transcendentals=0),
    )(*args)


def shifted(piece, axis, by):
    size = lax.axis_size(axis)
    return lax.ppermute(piece, axis, [(i, (i + by) % size) for i in range(size)])


def dealt(piece, dy):
    pairs = []
    for i in range(8):
        z0, y0, c = i // 4, i // 2 % 2, i % 2
        j = c * 4 + (y0 ^ dy) * 2 + z0
        if i != j:
            pairs.append((i, j))
    return lax.ppermute(piece, ("z0", "y0", "c"), pairs)


def between(piece, dy, s):
    pairs = []
    for i in range(32):
        z0, y0, x, c = i // 16, i // 8 % 2, i // 2 % 4, i % 2
        above = 1 - c if x >= 2 else c
        x_to, z_to, c_to = ((x + 1) % 4, c, above) if z0 ^ s else ((x + 3) % 4, above, c)
        pairs.append((i, z_to * 16 + (y0 ^ dy) * 8 + x_to * 2 + c_to))
    return lax.ppermute(piece, ("z0", "y0", "x", "c"), pairs)


def crossed(piece):
    return lax.ppermute(piece, ("x", "c"), [(4, 5), (5, 4), (6, 7), (7, 6)])


def steps(x):
    rows, cols = x.shape
    d = call(centre_kernel, shape(rows + 8, cols), (x,), flops=10**9, moved=2**21)
    up = shifted(d, "x", -1)
    down = shifted(d, "x", 1)
    swap = shifted(d, "c", 1)
    block = pltpu.VMEM((2, 4, 2, 32, cols), F32)
    mean = pltpu.VMEM((2, 8, cols), F32)
    t, *own = call(
        own_kernel,
        (shape(4 * cols, rows, dtype=BF16), *[shape(136, 2 * cols)] * 2),
        (d, swap),
        (block, mean),
        flops=2 * 10**9,
        moved=2**22,
    )
    cross = crossed(up)
    above = call(above_kernel, [shape(128, 2 * cols)] * 2, (t, up), (block,), flops=2 * 10**9, moved=2**22)
    near = call(near_kernel, [shape(264, 2 * cols)] * 2, (t, up, down, *above), (block,), flops=2 * 10**9, moved=2**22)
    far = call(far_kernel, [shape(136, cols)] * 4, (up, down, cross), (block, mean), flops=10**9, moved=2**22)
    far = [between(far[p], *divmod(p, 2)) for p in range(4)]
    sums = []
    for outs in (own, near):
        sums += [outs[0]] + [dealt(outs[dy], dy) for dy in range(2)]
    keep, send = call(
        merge_pair_kernel,
        [shape(392, cols)] * 2,
        sums,
        (pltpu.VMEM((2, 392, cols), F32),),
        flops=10**9,
        moved=2**22,
    )
    recv = shifted(send, "c", 1)
    merged = call(
        functools.partial(merge_block_kernel, rows),
        shape(16, 8, 4 * cols + 128),
        (keep, recv, *far),
        (pltpu.VMEM((4, 4, 2, 32, cols), F32),),
        flops=10**9,
        moved=2**22,
    )
    merged = lax.all_to_all(merged, ("z1", "y1"), 0, 0, tiled=True)
    covariance, mean = call(
        functools.partial(merge_all_kernel, 4 * rows),
        (shape(32, cols), shape(1, cols)),
        (merged,),
        (pltpu.VMEM((8, 4, 8, cols), F32),),
        flops=10**9,
        moved=2**20,
    )
    return covariance, mean.reshape(cols)


def solution(mesh):
    finer = Mesh(mesh.devices.reshape(4, 2, 4, 2, 4, 2), SCEN + FAC)
    return jax.shard_map(
        steps,
        mesh=finer,
        in_specs=(P(SCEN, FAC),),
        out_specs=(P(SCEN, FAC), P(FAC)),
        check_vma=False,
    )
```

```python
import functools

import jax
import jax.numpy as jnp
from jax import lax
from jax.experimental import pallas as pl
from jax.experimental.pallas import tpu as pltpu
from jax.sharding import Mesh
from jax.sharding import PartitionSpec as P


SCEN = ("z1", "z0", "y1", "y0")
FAC = ("x", "c")
VMEM = pl.BlockSpec(memory_space=pltpu.VMEM)
F32 = jnp.float32
BF16 = jnp.bfloat16


def shape(*dims, dtype=F32):
    return jax.ShapeDtypeStruct(dims, dtype)


def split(value):
    high = value.astype(BF16)
    return high, (value - high.astype(F32)).astype(BF16)


def outer(left, right):
    def product(one, two):
        return lax.dot_general(one, two, (((0,), (0,)), ((), ())), preferred_element_type=F32)

    left_high, left_low = split(left)
    right_high, right_low = split(right)
    return product(left_high, right_high) + (product(left_low, right_high) + product(left_high, right_low))


def centre_kernel(x_ref, d_ref):
    rows, cols = x_ref.shape
    mean = jnp.sum(x_ref[...], axis=0, keepdims=True) * (1.0 / rows)
    d_ref[0:rows, :] = x_ref[...] - mean
    d_ref[rows : rows + 8, :] = jnp.broadcast_to(mean, (8, cols))


def turn(piece, t_ref, at):
    cols = piece.shape[1]
    high, low = split(piece.T)
    t_ref[at : at + cols, :] = high
    t_ref[at + 2 * cols : at + 3 * cols, :] = low


def against(t_ref, left):
    high, low = split(left)
    two = t_ref.shape[0] // 2
    both = jnp.dot(t_ref[...], high, preferred_element_type=F32)
    rest = jnp.dot(t_ref[0:two, :], low, preferred_element_type=F32)
    return both[0:two] + (both[two:] + rest)


def deal(total, block, outs, at):
    cols = total.shape[1]
    y0, c = lax.axis_index("y0"), lax.axis_index("c")
    block[c] = total[0:cols].T.reshape(4, 2, 32, cols)
    block[1 - c] = total[cols:].T.reshape(4, 2, 32, cols)
    for dy in range(2):
        to = (1 - y0) if dy else y0
        for y1 in range(4):
            for j in range(2):
                lo = at + 32 * y1
                outs[dy][lo : lo + 32, cols * j : cols * j + cols] = block[j, y1, to]


def own_kernel(d_ref, s_ref, t_ref, *refs):
    outs, (block, mean) = refs[:2], refs[2:]
    cols = d_ref.shape[1]
    rows = d_ref.shape[0] - 8
    c = lax.axis_index("c")
    turn(d_ref[0:rows, :], t_ref, 0)
    turn(s_ref[0:rows, :], t_ref, cols)
    deal(against(t_ref, d_ref[0:rows, :]), block, outs, 0)
    mean[c] = d_ref[rows : rows + 8, :]
    mean[1 - c] = s_ref[rows : rows + 8, :]
    for out in outs:
        out[128:136, :] = jnp.zeros((8, 2 * cols), F32)
        for j in range(2):
            out[128:129, cols * j : cols * j + cols] = mean[j, 0:1, :]
        out[129:130, 0:cols] = d_ref[rows : rows + 1, :]


def above_kernel(t_ref, up_ref, *refs):
    outs, block = refs[:2], refs[2]
    rows = up_ref.shape[0] - 8
    deal(against(t_ref, up_ref[0:rows, :]), block, outs, 0)


def near_kernel(t_ref, up_ref, down_ref, *refs):
    above, outs, block = refs[:2], refs[2:4], refs[4]
    rows, cols = up_ref.shape[0] - 8, up_ref.shape[1]
    deal(against(t_ref, down_ref[0:rows, :]), block, outs, 128)
    for part, out in zip(above, outs, strict=True):
        out[0:128, :] = part[...]
        out[256:264, :] = jnp.zeros((8, 2 * cols), F32)
        for k, ref in enumerate((up_ref, down_ref)):
            out[256 + k : 257 + k, 0:cols] = ref[rows : rows + 1, :]


def far_kernel(up_ref, down_ref, cross_ref, *refs):
    outs, (block, mean) = refs[:4], refs[4:]
    rows, cols = up_ref.shape[0] - 8, up_ref.shape[1]
    z0, y0 = lax.axis_index("z0"), lax.axis_index("y0")
    crossed = jnp.full((1, cols), lax.axis_index("x") < 2)
    above = jnp.where(crossed, cross_ref[...], up_ref[...])
    high, low = split(above[0:rows].T)
    right_high, right_low = split(down_ref[0:rows, :])
    product = jnp.dot(high, right_high, preferred_element_type=F32) + (
        jnp.dot(low, right_high, preferred_element_type=F32) + jnp.dot(high, right_low, preferred_element_type=F32)
    )
    block[0] = product.reshape(4, 2, 32, cols)
    block[1] = product.T.reshape(4, 2, 32, cols)
    mean[0] = above[rows : rows + 8]
    mean[1] = down_ref[rows : rows + 8, :]
    for p, out in enumerate(outs):
        dy, s = divmod(p, 2)
        kind = (1 - z0) if s else z0
        to = (1 - y0) if dy else y0
        for y1 in range(4):
            out[32 * y1 : 32 * y1 + 32, :] = block[kind, y1, to]
        out[128:129, :] = mean[kind, 0:1, :]
        out[129:130, :] = mean[1 - kind, 0:1, :]
        out[130:136, :] = jnp.zeros((6, cols), F32)


def merge_pair_kernel(*refs):
    groups = (refs[0:3], refs[3:6])
    keep_ref, send_ref, parts = refs[6:]
    cols = keep_ref.shape[1]
    z0, c = lax.axis_index("z0"), lax.axis_index("c")
    kept = jnp.full((1, 2 * cols), z0 == c)

    def read(group, lo, n):
        return jnp.where(kept, group[0][lo : lo + n, :], group[1][lo : lo + n, :]), group[2][lo : lo + n, :]

    def put(lo, value):
        n = value.shape[0]
        for j in range(2):
            parts[j, lo : lo + n, :] = value[:, cols * j : cols * j + cols]

    for group, n, at in zip(groups, (1, 2), (0, 128), strict=True):
        one, two = read(group, 0, 128 * n)
        put(at, one + two)
    own = read(groups[0], 128, 8)
    near = read(groups[1], 256, 8)
    for dy in range(2):
        put(384 + dy, own[dy][0:1, :])
        for k, m in enumerate((own[dy][1:2, :], near[dy][0:1, :], near[dy][1:2, :])):
            for j in range(2):
                parts[j, 386 + 2 * k + dy : 387 + 2 * k + dy, :] = m[:, 0:cols]
    keep_ref[...] = parts[c]
    send_ref[...] = parts[1 - c]


def merge_block_kernel(count, keep_ref, recv_ref, *refs):
    far, (out_ref, shift) = refs[:4], refs[4:]
    cols = keep_ref.shape[1]
    x, y0 = lax.axis_index("x"), lax.axis_index("y0")
    zeros = jnp.zeros((4, cols), F32)

    def mean_of(means):
        return jnp.sum(means, axis=0, keepdims=True) * 0.25

    def pairs(lo):
        return jnp.concatenate([keep_ref[lo : lo + 2, :], recv_ref[lo : lo + 2, :]], axis=0)

    own_means = pairs(384)
    own_mean = mean_of(own_means)
    far_means = jnp.concatenate([f[129:130, :] for f in far], axis=0)
    right = jnp.concatenate([own_means - own_mean, far_means - own_mean], axis=0)
    row_means, left = [], []
    for k in range(4):
        means = pairs(386 + 2 * k) if k < 3 else jnp.concatenate([f[128:129, :] for f in far], axis=0)
        mean = mean_of(means)
        row_means.append(mean)
        left.append(jnp.concatenate([means - mean, zeros] if k < 3 else [zeros, means - mean], axis=0))
    moved = outer(jnp.concatenate(left, axis=1), right) * float(count)
    shift[...] = moved.reshape(4, 4, 2, 32, cols)
    for k, step in enumerate((0, 1, 3, 2)):
        to = lax.rem(x + step, 4)
        for y1 in range(4):
            if k < 3:
                lo = 128 * k + 32 * y1
                total = keep_ref[lo : lo + 32, :] + recv_ref[lo : lo + 32, :]
            else:
                lo = 32 * y1
                total = (far[0][lo : lo + 32, :] + far[1][lo : lo + 32, :]) + (
                    far[2][lo : lo + 32, :] + far[3][lo : lo + 32, :]
                )
            total = total + shift[k, y1, y0]
            for g in range(4):
                out_ref[4 * to + y1, :, cols * g : cols * g + cols] = total[8 * g : 8 * g + 8, :]
            for row, m in ((0, own_mean), (2, row_means[k])):
                for h in range(2):
                    out_ref[4 * to + y1, row + h : row + h + 1, 4 * cols :] = m[:, 128 * h : 128 * h + 128]
            out_ref[4 * to + y1, 4:8, 4 * cols :] = jnp.zeros((4, 128), F32)


def merge_all_kernel(count, in_ref, cov_ref, mean_ref, shift):
    blocks = in_ref.shape[0]
    cols = cov_ref.shape[1]
    total = in_ref[0]
    for s in range(1, blocks):
        total = total + in_ref[s]

    def means(row):
        halves = [
            jnp.concatenate([in_ref[s, row + h : row + h + 1, 4 * cols :] for s in range(blocks)], axis=0)
            for h in range(2)
        ]
        return jnp.concatenate(halves, axis=1)

    own, other = means(0), means(2)
    own_mean = jnp.sum(own, axis=0, keepdims=True) * (1.0 / blocks)
    other_mean = jnp.sum(other, axis=0, keepdims=True) * (1.0 / blocks)
    y = 2 * lax.axis_index("y1") + lax.axis_index("y0")
    shift[...] = (outer(other - other_mean, own - own_mean) * float(count)).reshape(8, 4, 8, cols)
    for g in range(4):
        here = total[:, cols * g : cols * g + cols] + shift[y, g]
        cov_ref[8 * g : 8 * g + 8, :] = here / float(count * blocks - 1)
    mean_ref[...] = own_mean


def call(kernel, outs, args, scratch=(), mib=16, flops=0, moved=0):
    return pl.pallas_call(
        kernel,
        out_shape=outs,
        in_specs=[VMEM] * len(args),
        out_specs=jax.tree.map(lambda _: VMEM, outs),
        scratch_shapes=scratch,
        compiler_params=pltpu.CompilerParams(vmem_limit_bytes=mib * 2**20),
        cost_estimate=pl.CostEstimate(flops=flops, bytes_accessed=moved, transcendentals=0),
    )(*args)


def shifted(piece, axis, by):
    size = lax.axis_size(axis)
    return lax.ppermute(piece, axis, [(i, (i + by) % size) for i in range(size)])


def dealt(piece, dy):
    pairs = []
    for i in range(8):
        z0, y0, c = i // 4, i // 2 % 2, i % 2
        j = c * 4 + (y0 ^ dy) * 2 + z0
        if i != j:
            pairs.append((i, j))
    return lax.ppermute(piece, ("z0", "y0", "c"), pairs)


def between(piece, dy, s):
    pairs = []
    for i in range(32):
        z0, y0, x, c = i // 16, i // 8 % 2, i // 2 % 4, i % 2
        above = 1 - c if x < 2 else c
        x_to, z_to, c_to = ((x + 1) % 4, c, above) if z0 ^ s else ((x + 3) % 4, above, c)
        pairs.append((i, z_to * 16 + (y0 ^ dy) * 8 + x_to * 2 + c_to))
    return lax.ppermute(piece, ("z0", "y0", "x", "c"), pairs)


def crossed(piece):
    return lax.ppermute(piece, ("x", "c"), [(0, 1), (1, 0), (2, 3), (3, 2)])


def steps(x):
    rows, cols = x.shape
    d = call(centre_kernel, shape(rows + 8, cols), (x,), flops=10**9, moved=2**21)
    up = shifted(d, "x", -1)
    down = shifted(d, "x", 1)
    swap = shifted(d, "c", 1)
    block = pltpu.VMEM((2, 4, 2, 32, cols), F32)
    mean = pltpu.VMEM((2, 8, cols), F32)
    t, *own = call(
        own_kernel,
        (shape(4 * cols, rows, dtype=BF16), *[shape(136, 2 * cols)] * 2),
        (d, swap),
        (block, mean),
        flops=2 * 10**9,
        moved=2**22,
    )
    cross = crossed(up)
    above = call(above_kernel, [shape(128, 2 * cols)] * 2, (t, up), (block,), flops=2 * 10**9, moved=2**22)
    near = call(near_kernel, [shape(264, 2 * cols)] * 2, (t, up, down, *above), (block,), flops=2 * 10**9, moved=2**22)
    far = call(far_kernel, [shape(136, cols)] * 4, (up, down, cross), (block, mean), flops=10**9, moved=2**22)
    far = [between(far[p], *divmod(p, 2)) for p in range(4)]
    sums = []
    for outs in (own, near):
        sums += [outs[0]] + [dealt(outs[dy], dy) for dy in range(2)]
    keep, send = call(
        merge_pair_kernel,
        [shape(392, cols)] * 2,
        sums,
        (pltpu.VMEM((2, 392, cols), F32),),
        flops=10**9,
        moved=2**22,
    )
    recv = shifted(send, "c", 1)
    merged = call(
        functools.partial(merge_block_kernel, rows),
        shape(16, 8, 4 * cols + 128),
        (keep, recv, *far),
        (pltpu.VMEM((4, 4, 2, 32, cols), F32),),
        flops=10**9,
        moved=2**22,
    )
    merged = lax.all_to_all(merged, ("z1", "y1"), 0, 0, tiled=True)
    covariance, mean = call(
        functools.partial(merge_all_kernel, 4 * rows),
        (shape(32, cols), shape(1, cols)),
        (merged,),
        (pltpu.VMEM((8, 4, 8, cols), F32),),
        flops=10**9,
        moved=2**20,
    )
    return covariance, mean.reshape(cols)


def solution(mesh):
    finer = Mesh(mesh.devices.reshape(4, 2, 4, 2, 4, 2), SCEN + FAC)
    return jax.shard_map(
        steps,
        mesh=finer,
        in_specs=(P(SCEN, FAC),),
        out_specs=(P(SCEN, FAC), P(FAC)),
        check_vma=False,
    )
```
